32 devices in a mesh: node: 16 (over z, y, core), blk: 2 (over x).
Axes of the slice: x: 2, y: 2, z: 4, core: 2. Of those that a mesh axis runs over, the one named last changes fastest.
Arguments:
- params: bfloat16 [16, 128, 14336], P('node', 'blk'), may hold values from -40 to 40
- weights: int32 [16], P('node'), may hold values from 1 to 8
Outputs:
- debiased: float32 [16, 128, 14336], P('node', 'blk')
- average: float32 [128, 14336], P('blk', 'node')
- spread: float32 [16], P('node')
The draws below stay inside these ranges and needn't reach their ends.
All inputs are finite; a program needn't handle non-finite values.
Results may differ from the reference program's by a relative error of at most 0.0003.
Values may be sent and summed in bfloat16 or wider, within the bound.
A program may use at most 64 MiB of HBM per device.

```python
import jax
import jax.numpy as jnp

FF = 14336
ROUNDS = 3
ROWS = 128
NODES = 16


def draw_params(key, part):
    keys = jax.random.split(jax.random.fold_in(key, 11), 3)
    index = jnp.arange(NODES, dtype=jnp.float32)
    node_scale = (1.0 + 2.0 * index / max(NODES - 1, 1)) * jax.random.uniform(keys[1], (NODES,), minval=0.8, maxval=1.2)
    base = jax.random.normal(keys[0], (NODES, ROWS, FF))
    row_scale = jnp.exp(jax.random.uniform(keys[2], (ROWS,), minval=0.0, maxval=jnp.log(3.0)))
    values = base * node_scale[:, None, None] * row_scale[None, :, None]
    return jnp.clip(values, -40.0, 40.0).astype(jnp.bfloat16)


def touch_ends(entries, key, least, largest):
    extent = entries.shape
    spot = [jax.random.randint(jax.random.fold_in(key, axis), (), 0, extent[axis]) for axis in range(len(extent))]
    entries = entries.at[tuple(spot)].set(least)
    longest = extent.index(max(extent))
    spot[longest] = (spot[longest] + 1) % extent[longest]
    return entries.at[tuple(spot)].set(largest)


def setup_inputs(seed: int = 0) -> dict:
    streams_of = jax.random.split(jax.random.key(seed), 3)
    return {
        "params": draw_params(jax.random.fold_in(streams_of[2], 71), 0),
        "weights": touch_ends(jax.random.randint(streams_of[1], (NODES,), 1, 9), jax.random.fold_in(streams_of[1], 1), 1, 8).astype(jnp.int32),
    }


def reference(params, weights):
    scale0 = weights.astype(jnp.float32)
    value = scale0[:, None, None] * params.astype(jnp.float32)
    scale = scale0
    levels = NODES.bit_length() - 1
    for step in range(ROUNDS):
        hop = 1 << (step % levels)
        value = 0.5 * value + 0.5 * jnp.roll(value, hop, 0)
        scale = 0.5 * scale + 0.5 * jnp.roll(scale, hop, 0)
    debiased = value / scale[:, None, None]
    numer = jnp.sum(scale0[:, None, None] * params.astype(jnp.float32), axis=0)
    average = numer / jnp.sum(scale0)
    spread = jnp.sum((debiased - average[None]) ** 2, axis=(1, 2)) / (ROWS * FF)
    return debiased, average, spread
```

```python
import functools

import jax
import jax.numpy as jnp
from jax import lax
from jax.experimental import pallas as pl
from jax.experimental.pallas import tpu as pltpu
from jax.sharding import PartitionSpec as P

ROUNDS = 3
GROUP = 4
LEVELS = 4
SPLIT = 4
LANES = 128
AHEAD = 4
NEIGHBOUR = (1, 0, 3, 2)


def kernel(p_ref, w_ref, out_ref, avg_ref, spread_ref,
           raw_own, raw_a, raw_b, raw_c, q_in, q_out, dbuf, avgbuf,
           wts, acc, part, spread_in,
           near_send, near_recv, own_sem, back_send, back_recv, back_own,
           piece_send, piece_recv, far_send, far_recv,
           w_send, w_recv, s_send, s_recv, avg_send, avg_recv):
    node = lax.axis_index("node")
    side = lax.axis_index("blk")
    z = node // GROUP
    r = node % GROUP
    half, core = r // 2, r % 2
    chunks, _, rows, width = raw_own.shape
    hidden = p_ref.shape[2]
    row_total = p_ref.shape[1] * lax.axis_size("blk")
    middle = chunks // 2

    lows = list(range(middle))
    highs = list(range(middle + SPLIT, chunks)) + list(range(middle, middle + SPLIT))
    order = [k for pair in zip(lows, highs) for k in pair]
    first = order[:AHEAD]

    def peer(o):
        y = 1 - half if o & 2 else half
        c = 1 - core if o & 1 else core
        return y * 2 + c

    def dev(zz, rr):
        return {"node": zz * GROUP + rr}

    inner = jnp.logical_and(z >= 1, z <= 2)
    mate = 3 - z
    nb = (z // 2) * 2 + 1 - z % 2
    inner_count = (1 - z // 3) * ((z + 2) // 3)

    def remote(src, dst, ssem, rsem, device):
        return pltpu.make_async_remote_copy(
            src_ref=src, dst_ref=dst, send_sem=ssem, recv_sem=rsem,
            device_id=device, device_id_type=pl.DeviceIdType.MESH)

    def own_slice(k):
        return pl.ds((k % SPLIT) * rows, rows)

    def block(k, rr):
        return pl.ds(pl.multiple_of(((k // SPLIT) * GROUP + rr) * width, LANES), width)

    barrier = pltpu.get_barrier_semaphore()

    def greet(device):
        pl.semaphore_signal(barrier, inc=1, device_id=device,
                            device_id_type=pl.DeviceIdType.MESH)

    for o in (1, 2, 3):
        greet(dev(z, peer(o)))
    greet({"blk": 1 - side})
    greet(dev(nb, r))

    @pl.when(inner)
    def _():
        greet(dev(mate, r))

    def local_in(k):
        return pltpu.make_async_copy(
            p_ref.at[0, own_slice(k), block(k, r)], raw_own.at[k, r], own_sem.at[k])

    for k in order:
        local_in(k).start()
    wts[z, r] = jnp.full((8, LANES), w_ref[0].astype(jnp.float32))
    acc[...] = jnp.zeros_like(acc)

    pl.semaphore_wait(barrier, 5 + inner_count)

    def w_near(o):
        return remote(wts.at[z, r], wts.at[z, r], w_send.at[o - 1], w_recv.at[o - 1],
                      dev(z, peer(o)))

    def near(k, o):
        return remote(p_ref.at[0, own_slice(k), block(k, peer(o))], raw_own.at[k, r],
                      near_send.at[k, o - 1], near_recv.at[k, o - 1], dev(z, peer(o)))

    def send_near(ks):
        for k in ks:
            for o in (2, 3, 1):
                near(k, o).start()

    arrived = set()

    def wait_piece(k, o):
        if (k, o) in arrived:
            return
        arrived.add((k, o))
        if o:
            near(k, o).wait_recv()
        else:
            local_in(k).wait()

    def wait_own(k):
        for o in range(GROUP):
            wait_piece(k, o)

    def row(zz, i):
        return wts[zz, i, 0:1, :]

    def value(ref, k, zz, i, cols):
        return ref[k, i, :, cols].astype(jnp.float32) * row(zz, i)

    def group_sum(ref, k, zz, cols):
        return ((value(ref, k, zz, 0, cols) + value(ref, k, zz, 1, cols))
                + (value(ref, k, zz, 2, cols) + value(ref, k, zz, 3, cols)))

    def columns(j):
        return pl.ds(pl.multiple_of(j * LANES, LANES), LANES)

    def back(k, o):
        return remote(dbuf.at[k, peer(o)], out_ref.at[0, own_slice(k), block(k, r)],
                      back_send.at[k, o - 1], back_recv.at[k, o - 1], dev(z, peer(o)))

    def back_local(k):
        return pltpu.make_async_copy(
            dbuf.at[k, r], out_ref.at[0, own_slice(k), block(k, r)], back_own.at[k])

    def send_back(k):
        for o in (2, 3, 1):
            back(k, o).start()
        back_local(k).start()

    def group_weight(zz):
        return row(zz, 0) + row(zz, 1) + row(zz, 2) + row(zz, 3)

    def scales_of(level):
        opp = (level + 2) % LEVELS
        sums = [group_weight((level + 3) % LEVELS)] * GROUP
        for i in range(GROUP):
            for e in range(GROUP):
                sums[i] = sums[i] + row(level if e <= i else opp, e)
        return [1.0 / total for total in sums]

    def window(own, tail, prior):
        heads = [own[0]]
        for i in range(1, GROUP):
            heads.append(heads[-1] + own[i])
        tails = [None, None, None, tail[3]]
        for i in (2, 1):
            tails[i] = tails[i + 1] + tail[i]
        sums = [head + prior for head in heads]
        return [sums[i] + tails[i + 1] for i in range(GROUP - 1)] + [sums[-1]]

    def debias(k, level, prior_ref, tail_ref):
        opp, prior_level = (level + 2) % LEVELS, (level + 3) % LEVELS
        scales = scales_of(level)

        def step(j, carry):
            cols = columns(j)
            if prior_ref is None:
                prior = q_in[k, :, cols]
            else:
                prior = group_sum(prior_ref, k, prior_level, cols)
            own = [value(raw_own, k, level, i, cols) for i in range(GROUP)]
            tail = [None] + [value(tail_ref, k, opp, i, cols) for i in range(1, GROUP)]
            for i, total in enumerate(window(own, tail, prior)):
                dbuf[k, i, :, cols] = total * scales[i]
            return carry

        lax.fori_loop(0, width // LANES, step, 0)

    def means(k, level):
        refs = {level: raw_own, NEIGHBOUR[level]: raw_a, 3 - level: raw_b,
                (level + 2) % LEVELS: raw_c}
        slot = 1 if k // SPLIT == level else 0
        whole = 1.0 / (group_weight(0) + group_weight(1) + group_weight(2) + group_weight(3))
        scales = [scales_of(y) for y in range(LEVELS)]

        def step(j, sums):
            cols = columns(j)
            groups = [group_sum(refs[y], k, y, cols) for y in range(LEVELS)]
            mean = ((groups[0] + groups[1]) + (groups[2] + groups[3])) * whole
            avgbuf[slot, own_slice(k), cols] = mean
            fresh = []
            for y in range(LEVELS):
                far = (y + 2) % LEVELS
                own = [value(refs[y], k, y, i, cols) for i in range(GROUP)]
                tail = [None] + [value(refs[far], k, far, i, cols) for i in range(1, GROUP)]
                for i, total in enumerate(window(own, tail, groups[(y + 3) % LEVELS])):
                    gap = total * scales[y][i] - mean
                    gap = gap * gap
                    fold = gap[0:8]
                    for e in range(8, rows, 8):
                        fold = fold + gap[e:e + 8]
                    fresh.append(sums[y * GROUP + i] + fold)
            return tuple(fresh)

        zero = jnp.zeros((8, LANES), jnp.float32)
        sums = lax.fori_loop(0, width // LANES, step, (zero,) * (LEVELS * GROUP))
        for y in range(LEVELS):
            for i in range(GROUP):
                acc[y, i] += sums[y * GROUP + i]

    def nodes(full):
        return pl.ds(0, GROUP) if full else pl.ds(1, GROUP - 1)

    def to_inner(k, beside):
        return remote(raw_own.at[k], raw_a.at[k], far_send.at[k, 0], far_recv.at[k, 0],
                      dev(beside, r))

    def piece(k, o, source):
        n = first.index(k)
        return remote(raw_own.at[k, peer(o)], raw_b.at[k, peer(o)], piece_send.at[n, o],
                      piece_recv.at[n, o], dev(3 - source, r))

    def with_piece(k, o, source, act):
        if source == 1 or k < middle:
            act()
        else:
            pl.when(peer(o) != 0)(act)

    def across(k, source):
        part_of = nodes(source == 1)
        return remote(raw_own.at[k, part_of], raw_b.at[k, part_of], far_send.at[k, 0],
                      far_recv.at[k, 1], dev(3 - source, r))

    def across_wait(k, source, sent):
        if k not in first:
            copy = across(k, source)
            copy.wait_send() if sent else copy.wait_recv()
            return
        for o in range(GROUP):
            copy = piece(k, o, source)
            with_piece(k, o, source, copy.wait_send if sent else copy.wait_recv)

    def across_relay(k, source):
        part_of = nodes(source == 2)
        return remote(raw_a.at[k, part_of], raw_c.at[k, part_of], far_send.at[k, 1],
                      far_recv.at[k, 2], dev(3 - source, r))

    def extra(k, source):
        n = k % middle
        if source == 1:
            src, dst = raw_a, raw_c
        else:
            src, dst = raw_own, raw_b
        return remote(src.at[k, 0], dst.at[k, 0], far_send.at[n, 4], far_recv.at[n, 4],
                      dev(3 - source, r))

    def outward_relay(k, source):
        part_of = nodes(False)
        return remote(raw_b.at[k, part_of], raw_a.at[k, part_of], far_send.at[k, 2],
                      far_recv.at[k, 0], dev(NEIGHBOUR[source], r))

    def outward_q(k, source):
        return remote(q_out.at[k], q_in.at[k], far_send.at[k, 3], far_recv.at[k, 3],
                      dev(NEIGHBOUR[source], r))

    def outward_mean(k, source):
        n = k % SPLIT
        return remote(avgbuf.at[0, own_slice(k)], avg_ref.at[own_slice(k)],
                      avg_send.at[n], avg_recv.at[n], dev(NEIGHBOUR[source], r))

    def own_mean(k):
        n = k % SPLIT
        return pltpu.make_async_copy(
            avgbuf.at[1, own_slice(k)], avg_ref.at[own_slice(k)], avg_recv.at[n])

    def w_copy(level, slot, target):
        return remote(wts.at[level], wts.at[level], w_send.at[slot], w_recv.at[slot],
                      dev(target, r))

    def spread_slot(level, x, rr):
        return (level - 1) * 2 * GROUP + x * GROUP + rr

    def share(level, y, o, flip):
        x = 1 - side if flip else side
        return remote(part.at[y, peer(o)], spread_in.at[spread_slot(level, side, r)],
                      s_send.at[y, o, flip], s_recv.at[spread_slot(level, side, r)],
                      {"node": y * GROUP + peer(o), "blk": x})

    def shares(level):
        return [(y, o, flip) for y in (3 - level, (level + 2) % LEVELS, NEIGHBOUR[level], level)
                for flip in (1, 0) for o in (3, 2, 1, 0) if y != level or flip or o]

    def gather_spread(level):
        for maker in (1, 2):
            for flip in (0, 1):
                x = 1 - side if flip else side
                for o in range(GROUP):
                    if maker == level and not flip and not o:
                        continue
                    slot = spread_slot(maker, x, peer(o))
                    remote(part.at[0, 0], spread_in.at[slot], s_send.at[0, 0, 0],
                           s_recv.at[slot], {"blk": 1 - side}).wait_recv()

    def inner_role(level):
        beside, other, opp = NEIGHBOUR[level], 3 - level, (level + 2) % LEVELS
        arrived.clear()
        sent_extras = [k for k in (highs if level == 1 else lows)
                       if level == 1 or k not in first]
        mine = lows if level == 1 else highs
        prior_ref = raw_a if level == 1 else raw_b

        def make_q(k):
            src, zz = (raw_c, opp) if level == 1 else (raw_own, level)

            def step(j, carry):
                cols = columns(j)
                q_out[k, :, cols] = group_sum(src, k, zz, cols)
                return carry

            lax.fori_loop(0, width // LANES, step, 0)
            outward_q(k, level).start()

        for k in first:
            wait_piece(k, 0)
            with_piece(k, 0, level, piece(k, 0, level).start)
        send_near(first)
        for o in (1, 2, 3):
            w_near(o).start()
        send_near(order[AHEAD:])
        for k in first:
            wait_piece(k, 1)
            with_piece(k, 1, level, piece(k, 1, level).start)
        for n, k in enumerate(first):
            for o in (2, 3):
                wait_piece(k, o)
                with_piece(k, o, level, piece(k, o, level).start)
            if n == 0:
                for o in (1, 2, 3):
                    w_near(o).wait_recv()
                w_copy(level, 3, beside).start()
                w_copy(level, 4, other).start()

        for t in range(chunks + 2):
            if t + AHEAD < chunks:
                wait_own(order[t + AHEAD])
                across(order[t + AHEAD], level).start()
            if t < chunks:
                k = order[t]
                to_inner(k, beside).wait_recv()
                across_relay(k, level).start()
                if t == 0:
                    w_copy(beside, 3, beside).wait_recv()
                    w_copy(beside, 5, other).start()
                    w_copy(level, 4, other).wait_recv()
                    w_copy(other, 6, beside).start()
                if t == chunks - 1:
                    for e in sent_extras:
                        extra(e, level).start()
                if level == 2:
                    make_q(k)
                across_wait(k, other, False)
                outward_relay(k, level).start()
            if t == 2:
                w_copy(opp, 5, other).wait_recv()
                w_copy(opp, 7, beside).start()
            if t >= 2:
                k = order[t - 2]
                across_relay(k, other).wait_recv()
                if level == 1:
                    make_q(k)
                debias(k, level, prior_ref, raw_c)
                send_back(k)
        for k in mine:
            if level == 2 or k not in first:
                extra(k, other).wait_recv()
            means(k, level)
            if k // SPLIT == level:
                own_mean(k).start()
            else:
                outward_mean(k, level).start()
        for y in range(LEVELS):
            for i in range(GROUP):
                part[y, i] = jnp.sum(acc[y, i], axis=0, keepdims=True)
        for y, o, flip in shares(level):
            share(level, y, o, flip).start()
        spread_in[spread_slot(level, side, r)] = part[level, r]

        for k in order:
            across_wait(k, level, True)
            across_relay(k, level).wait_send()
            outward_relay(k, level).wait_send()
            outward_q(k, level).wait_send()
        for k in sent_extras:
            extra(k, level).wait_send()
        w_copy(level, 3, beside).wait_send()
        w_copy(level, 4, other).wait_send()
        w_copy(beside, 5, other).wait_send()
        w_copy(other, 6, beside).wait_send()
        w_copy(opp, 7, beside).wait_send()
        for k in mine:
            if k // SPLIT == level:
                own_mean(k).wait()
            else:
                outward_mean(k, level).wait_send()
        gather_spread(level)
        for y, o, flip in shares(level):
            share(level, y, o, flip).wait_send()

    def outer_role(level):
        beside, other, opp = NEIGHBOUR[level], 3 - level, (level + 2) % LEVELS
        arrived.clear()
        send_near(first)
        for o in (1, 2, 3):
            w_near(o).start()
        send_near(order[AHEAD:])
        for n, k in enumerate(order):
            wait_own(k)
            to_inner(k, beside).start()
            if n == 0:
                for o in (1, 2, 3):
                    w_near(o).wait_recv()
                w_copy(level, 3, beside).start()
        w_copy(beside, 3, beside).wait_recv()
        w_copy(opp, 6, beside).wait_recv()
        w_copy(other, 7, beside).wait_recv()
        for k in order:
            outward_relay(k, beside).wait_recv()
            outward_q(k, beside).wait_recv()
            debias(k, level, None, raw_a)
            send_back(k)
        for k in order:
            to_inner(k, beside).wait_send()
        w_copy(level, 3, beside).wait_send()
        for k in range(SPLIT):
            outward_mean(k + level * SPLIT, beside).wait_recv()
        gather_spread(level)

    for level in range(LEVELS):
        role = inner_role if level in (1, 2) else outer_role
        pl.when(z == level)(functools.partial(role, level))

    for k in order:
        for o in (1, 2, 3):
            near(k, o).wait_send()
            back(k, o).wait()
        back_local(k).wait()
    for o in (1, 2, 3):
        w_near(o).wait_send()
    total = spread_in[0]
    for slot in range(1, spread_in.shape[0]):
        total = total + spread_in[slot]
    spread_ref[0] = jnp.sum(total) / (row_total * hidden)


def fused(params, weights):
    _, rows, hidden = params.shape
    node_count = lax.axis_size("node")
    width = hidden // node_count
    piece_rows = rows // SPLIT
    chunks = LEVELS * SPLIT
    raw = pltpu.VMEM((chunks, GROUP, piece_rows, width), params.dtype)
    q = pltpu.VMEM((chunks, piece_rows, width), jnp.float32)
    dma = pltpu.SemaphoreType.DMA
    debiased, average, spread = pl.pallas_call(
        kernel,
        out_shape=(
            jax.ShapeDtypeStruct((1, rows, hidden), jnp.float32),
            jax.ShapeDtypeStruct((rows, width), jnp.float32),
            jax.ShapeDtypeStruct((1,), jnp.float32),
        ),
        in_specs=[pl.BlockSpec(memory_space=pltpu.HBM), pl.BlockSpec(memory_space=pltpu.SMEM)],
        out_specs=(pl.BlockSpec(memory_space=pl.ANY), pl.BlockSpec(memory_space=pl.ANY),
                   pl.BlockSpec(memory_space=pltpu.SMEM)),
        scratch_shapes=[
            raw, raw, raw, raw, q, q,
            pltpu.VMEM((chunks, GROUP, piece_rows, width), jnp.float32),
            pltpu.VMEM((2, rows, width), jnp.float32),
            pltpu.VMEM((LEVELS, GROUP, 8, LANES), jnp.float32),
            pltpu.VMEM((LEVELS, GROUP, 8, LANES), jnp.float32),
            pltpu.VMEM((LEVELS, GROUP, 1, LANES), jnp.float32),
            pltpu.VMEM((4 * GROUP, 1, LANES), jnp.float32),
            dma((chunks, 3)), dma((chunks, 3)), dma((chunks,)),
            dma((chunks, 3)), dma((chunks, 3)), dma((chunks,)),
            dma((AHEAD, GROUP)), dma((AHEAD, GROUP)),
            dma((chunks, 5)), dma((chunks, 5)),
            dma((8,)), dma((8,)), dma((LEVELS, GROUP, 2)), dma((4 * GROUP,)),
            dma((SPLIT,)), dma((SPLIT,)),
        ],
        compiler_params=pltpu.CompilerParams(
            collective_id=0, has_side_effects=True, vmem_limit_bytes=20 << 20),
    )(params, weights)
    return debiased, average, spread


def from_behind(value, axis, steps):
    count = lax.axis_size(axis)
    pairs = [(source, (source + steps) % count) for source in range(count)]
    return lax.ppermute(value, axis, pairs)


def push_round(value, scale, hop):
    received = from_behind((value, scale), "node", hop)
    return (received[0], received[1])


def shards(params, weights):
    node_count = lax.axis_size("node")
    levels = node_count.bit_length() - 1
    scale0 = weights.astype(jnp.float32)
    weighted = scale0[:, None, None] * params.astype(jnp.float32)
    value = weighted
    scale = scale0
    for step in range(ROUNDS):
        hop = 1 << step % levels
        if step == 0:
            raw = from_behind((params, weights.astype(jnp.bfloat16)), "node", hop)
            other_scale = raw[1].astype(jnp.float32)
            other_value = other_scale[:, None, None] * raw[0].astype(jnp.float32)
        else:
            other_value, other_scale = push_round(value, scale, hop)
        value = 0.5 * value + 0.5 * other_value
        scale = 0.5 * scale + 0.5 * other_scale
    debiased = value / scale[:, None, None]
    hidden_units = params.shape[2]
    width = hidden_units // node_count
    local = debiased[0]
    numer, total = lax.psum((weighted[0], jnp.sum(scale0)), "node")
    whole = numer / total
    partial_value = jnp.sum((local - whole) ** 2)[None]
    average = lax.dynamic_slice_in_dim(whole, lax.axis_index("node") * width, width, 1)
    row_count = params.shape[1] * lax.axis_size("blk")
    spread = lax.psum(partial_value, "blk") / (row_count * hidden_units)
    return (debiased, average, spread)


def solution(mesh):
    line = mesh.shape["node"] == GROUP * LEVELS and mesh.shape["blk"] == 2
    return jax.shard_map(
        fused if line else shards,
        mesh=mesh,
        in_specs=(P("node", "blk", None), P("node")),
        out_specs=(P("node", "blk", None), P("blk", "node"), P("node")),
        check_vma=False,
    )
```

```python
import functools

import jax
import jax.numpy as jnp
from jax import lax
from jax.experimental import pallas as pl
from jax.experimental.pallas import tpu as pltpu
from jax.sharding import PartitionSpec as P

ROUNDS = 3
GROUP = 4
LEVELS = 4
SPLIT = 4
LANES = 128
AHEAD = 2
LATE = 4
NEIGHBOUR = (1, 0, 3, 2)


def kernel(p_ref, w_ref, out_ref, avg_ref, spread_ref,
           raw_own, raw_a, raw_b, raw_c, q_in, q_out, dbuf, avgbuf,
           wts, acc, part, spread_in,
           near_send, near_recv, beside_recv, own_sem, back_send, back_recv, back_own,
           far_send, own_recv, relay_recv, beside_in, q_recv, extra_recv,
           w_send, w_recv, s_send, s_recv, avg_send, avg_recv):
    node = lax.axis_index("node")
    side = lax.axis_index("blk")
    z = node // GROUP
    r = node % GROUP
    half, core = r // 2, r % 2
    chunks, _, rows, width = raw_own.shape
    hidden = p_ref.shape[2]
    row_total = p_ref.shape[1] * lax.axis_size("blk")
    middle = chunks // 2

    lows = list(range(middle))
    highs = list(range(middle + SPLIT, chunks)) + list(range(middle, middle + SPLIT))
    order = [k for pair in zip(lows, highs) for k in pair]
    first = order[:AHEAD]

    def peer(o):
        y = 1 - half if o & 2 else half
        c = 1 - core if o & 1 else core
        return y * 2 + c

    def dev(zz, rr):
        return {"node": zz * GROUP + rr}

    inner = jnp.logical_and(z >= 1, z <= 2)
    mate = 3 - z
    nb = (z // 2) * 2 + 1 - z % 2
    inner_count = (1 - z // 3) * ((z + 2) // 3)

    def remote(src, dst, ssem, rsem, device):
        return pltpu.make_async_remote_copy(
            src_ref=src, dst_ref=dst, send_sem=ssem, recv_sem=rsem,
            device_id=device, device_id_type=pl.DeviceIdType.MESH)

    def drain(ref, sem):
        pltpu.make_async_copy(ref, ref, sem).wait()

    def own_slice(k):
        return pl.ds((k % SPLIT) * rows, rows)

    def block(k, rr):
        return pl.ds(pl.multiple_of(((k // SPLIT) * GROUP + rr) * width, LANES), width)

    barrier = pltpu.get_barrier_semaphore()

    def greet(device):
        pl.semaphore_signal(barrier, inc=1, device_id=device,
                            device_id_type=pl.DeviceIdType.MESH)

    for o in (1, 2, 3):
        greet(dev(z, peer(o)))
    greet({"blk": 1 - side})
    greet(dev(nb, r))

    @pl.when(inner)
    def _():
        greet(dev(mate, r))

    def local_in(k):
        return pltpu.make_async_copy(
            p_ref.at[0, own_slice(k), block(k, r)], raw_own.at[k, r], own_sem)

    for k in order:
        local_in(k).start()
    wts[z, r] = jnp.full((8, LANES), w_ref[0].astype(jnp.float32))
    acc[...] = jnp.zeros_like(acc)

    pl.semaphore_wait(barrier, 5 + inner_count)
    drain(raw_own.at[:, 0], own_sem)

    def w_near(o):
        return remote(wts.at[z, r], wts.at[z, r], w_send.at[0], w_recv.at[0],
                      dev(z, peer(o)))

    def near(k, o):
        return remote(p_ref.at[0, own_slice(k), block(k, peer(o))], raw_own.at[k, r],
                      near_send, beside_recv.at[first.index(k)] if k in first and o == 1
                      else near_recv.at[k], dev(z, peer(o)))

    def send_near(ks):
        for k in ks:
            for o in (2, 3, 1):
                near(k, o).start()

    def near_weights():
        drain(wts.at[0, pl.ds(0, GROUP - 1)], w_recv.at[0])

    def wait_beside(k):
        drain(raw_own.at[k, 0], beside_recv.at[first.index(k)])

    def wait_near(k):
        count = GROUP - 2 if k in first else GROUP - 1
        drain(raw_own.at[k, pl.ds(0, count)], near_recv.at[k])

    def row(zz, i):
        return wts[zz, i, 0:1, :]

    def value(ref, k, zz, i, cols):
        return ref[k, i, :, cols].astype(jnp.float32) * row(zz, i)

    def group_sum(ref, k, zz, cols):
        return ((value(ref, k, zz, 0, cols) + value(ref, k, zz, 1, cols))
                + (value(ref, k, zz, 2, cols) + value(ref, k, zz, 3, cols)))

    def columns(j):
        return pl.ds(pl.multiple_of(j * LANES, LANES), LANES)

    def back(k, o):
        return remote(dbuf.at[k, peer(o)], out_ref.at[0, own_slice(k), block(k, r)],
                      back_send, back_recv, dev(z, peer(o)))

    def back_local(k):
        return pltpu.make_async_copy(
            dbuf.at[k, r], out_ref.at[0, own_slice(k), block(k, r)], back_own)

    def send_back(k):
        for o in (2, 3, 1):
            back(k, o).start()
        back_local(k).start()

    def group_weight(zz):
        return row(zz, 0) + row(zz, 1) + row(zz, 2) + row(zz, 3)

    def scales_of(level):
        opp = (level + 2) % LEVELS
        sums = [group_weight((level + 3) % LEVELS)] * GROUP
        for i in range(GROUP):
            for e in range(GROUP):
                sums[i] = sums[i] + row(level if e <= i else opp, e)
        return [1.0 / total for total in sums]

    def window(own, tail, prior):
        heads = [own[0]]
        for i in range(1, GROUP):
            heads.append(heads[-1] + own[i])
        tails = [None, None, None, tail[3]]
        for i in (2, 1):
            tails[i] = tails[i + 1] + tail[i]
        sums = [head + prior for head in heads]
        return [sums[i] + tails[i + 1] for i in range(GROUP - 1)] + [sums[-1]]

    def debias(k, level, prior_ref, tail_ref):
        opp, prior_level = (level + 2) % LEVELS, (level + 3) % LEVELS
        scales = scales_of(level)

        def step(j, carry):
            cols = columns(j)
            if prior_ref is None:
                prior = q_in[k, :, cols]
            else:
                prior = group_sum(prior_ref, k, prior_level, cols)
            own = [value(raw_own, k, level, i, cols) for i in range(GROUP)]
            tail = [None] + [value(tail_ref, k, opp, i, cols) for i in range(1, GROUP)]
            for i, total in enumerate(window(own, tail, prior)):
                dbuf[k, i, :, cols] = total * scales[i]
            return carry

        lax.fori_loop(0, width // LANES, step, 0)

    def means(k, level):
        refs = {level: raw_own, NEIGHBOUR[level]: raw_a, 3 - level: raw_b,
                (level + 2) % LEVELS: raw_c}
        slot = 1 if k // SPLIT == level else 0
        whole = 1.0 / (group_weight(0) + group_weight(1) + group_weight(2) + group_weight(3))
        scales = [scales_of(y) for y in range(LEVELS)]

        def step(j, sums):
            cols = columns(j)
            groups = [group_sum(refs[y], k, y, cols) for y in range(LEVELS)]
            mean = ((groups[0] + groups[1]) + (groups[2] + groups[3])) * whole
            avgbuf[slot, own_slice(k), cols] = mean
            fresh = []
            for y in range(LEVELS):
                far = (y + 2) % LEVELS
                own = [value(refs[y], k, y, i, cols) for i in range(GROUP)]
                tail = [None] + [value(refs[far], k, far, i, cols) for i in range(1, GROUP)]
                for i, total in enumerate(window(own, tail, groups[(y + 3) % LEVELS])):
                    gap = total * scales[y][i] - mean
                    gap = gap * gap
                    fold = gap[0:8]
                    for e in range(8, rows, 8):
                        fold = fold + gap[e:e + 8]
                    fresh.append(sums[y * GROUP + i] + fold)
            return tuple(fresh)

        zero = jnp.zeros((8, LANES), jnp.float32)
        sums = lax.fori_loop(0, width // LANES, step, (zero,) * (LEVELS * GROUP))
        for y in range(LEVELS):
            for i in range(GROUP):
                acc[y, i] += sums[y * GROUP + i]

    def nodes(full):
        return pl.ds(0, GROUP) if full else pl.ds(1, GROUP - 1)

    def to_inner(k, beside):
        return remote(raw_own.at[k], raw_a.at[k], far_send.at[0], beside_in.at[k],
                      dev(beside, r))

    def piece(k, o, source):
        return remote(raw_own.at[k, peer(o)], raw_b.at[k, peer(o)],
                      far_send.at[6 if all_own(k, source) else 7], own_recv.at[k],
                      dev(3 - source, r))

    def all_own(k, source):
        return source == 1 or (k in first and k < middle)

    def send_piece(k, o, source):
        start = piece(k, o, source).start
        if all_own(k, source):
            start()
        else:
            pl.when(peer(o) != 0)(start)

    def across(k, source):
        part_of = nodes(source == 1)
        return remote(raw_own.at[k, part_of], raw_b.at[k, part_of], far_send.at[1],
                      own_recv.at[k], dev(3 - source, r))

    def across_wait(k, source):
        drain(raw_b.at[k, nodes(all_own(k, source))], own_recv.at[k])

    def across_sent(source):
        drain(raw_own.at[pl.ds(0, chunks - AHEAD), nodes(source == 1)], far_send.at[1])
        if source == 1:
            drain(raw_own.at[pl.ds(0, AHEAD)], far_send.at[6])
        else:
            drain(raw_own.at[pl.ds(0, AHEAD // 2)], far_send.at[6])
            drain(raw_own.at[pl.ds(0, AHEAD // 2), nodes(False)], far_send.at[7])

    def across_relay(k, source):
        part_of = nodes(source == 2)
        return remote(raw_a.at[k, part_of], raw_c.at[k, part_of], far_send.at[2],
                      relay_recv.at[k], dev(3 - source, r))

    def extra(k, source):
        if source == 1:
            src, dst = raw_a, raw_c
        else:
            src, dst = raw_own, raw_b
        return remote(src.at[k, 0], dst.at[k, 0], far_send.at[3], extra_recv.at[k % middle],
                      dev(3 - source, r))

    def outward_relay(k, source):
        part_of = nodes(False)
        return remote(raw_b.at[k, part_of], raw_a.at[k, part_of], far_send.at[4],
                      beside_in.at[k], dev(NEIGHBOUR[source], r))

    def outward_q(k, source):
        return remote(q_out.at[k], q_in.at[k], far_send.at[5], q_recv.at[k],
                      dev(NEIGHBOUR[source], r))

    def outward_mean(k, source):
        return remote(avgbuf.at[0, own_slice(k)], avg_ref.at[own_slice(k)],
                      avg_send, avg_recv, dev(NEIGHBOUR[source], r))

    def own_mean(k):
        return pltpu.make_async_copy(
            avgbuf.at[1, own_slice(k)], avg_ref.at[own_slice(k)], avg_recv)

    def w_copy(level, slot, target):
        return remote(wts.at[level], wts.at[level], w_send.at[slot], w_recv.at[slot],
                      dev(target, r))

    def spread_slot(level, x, rr):
        return (level - 1) * 2 * GROUP + x * GROUP + rr

    def share(level, y, o, flip):
        x = 1 - side if flip else side
        return remote(part.at[y, peer(o)], spread_in.at[spread_slot(level, side, r)],
                      s_send.at[flip], s_recv,
                      {"node": y * GROUP + peer(o), "blk": x})

    def shares(level):
        return [(y, o, flip) for y in (3 - level, (level + 2) % LEVELS, NEIGHBOUR[level], level)
                for flip in (1, 0) for o in (3, 2, 1, 0) if y != level or flip or o]

    def gather_spread(level):
        slots = spread_in.shape[0]
        drain(spread_in.at[pl.ds(0, slots - 1 if level in (1, 2) else slots)], s_recv)

    def inner_role(level):
        beside, other, opp = NEIGHBOUR[level], 3 - level, (level + 2) % LEVELS
        sent_extras = [k for k in (highs if level == 1 else lows)
                       if level == 1 or k not in first]
        late_sent = sent_extras[-LATE:]
        mine = lows if level == 1 else highs
        late_mine = mine[-LATE:]
        prior_ref = raw_a if level == 1 else raw_b

        def make_q(k):
            src, zz = (raw_c, opp) if level == 1 else (raw_own, level)

            def step(j, carry):
                cols = columns(j)
                q_out[k, :, cols] = group_sum(src, k, zz, cols)
                return carry

            lax.fori_loop(0, width // LANES, step, 0)
            outward_q(k, level).start()

        def make_mean(k):
            if level == 2 or k not in first:
                extra(k, other).wait_recv()
            means(k, level)
            if k // SPLIT == level:
                own_mean(k).start()
            else:
                outward_mean(k, level).start()

        for k in first:
            send_piece(k, 0, level)
        send_near(first)
        for o in (1, 2, 3):
            w_near(o).start()
        send_near(order[AHEAD:])
        for k in first:
            wait_beside(k)
            send_piece(k, 1, level)
        for n, k in enumerate(first):
            wait_near(k)
            for o in (2, 3):
                send_piece(k, o, level)
            if n == 0:
                near_weights()
                w_copy(level, 3, beside).start()
                w_copy(level, 4, other).start()

        for t in range(chunks + 2):
            if t + AHEAD < chunks:
                wait_near(order[t + AHEAD])
                across(order[t + AHEAD], level).start()
            if t < chunks:
                k = order[t]
                to_inner(k, beside).wait_recv()
                across_relay(k, level).start()
                if k in sent_extras and k not in late_sent:
                    extra(k, level).start()
                if t == 0:
                    w_copy(beside, 3, beside).wait_recv()
                    w_copy(beside, 5, other).start()
                    w_copy(level, 4, other).wait_recv()
                    w_copy(other, 6, beside).start()
                if t == chunks - 1:
                    for e in late_sent:
                        extra(e, level).start()
                if level == 2:
                    make_q(k)
                across_wait(k, other)
                outward_relay(k, level).start()
            if t == 2:
                w_copy(opp, 5, other).wait_recv()
                w_copy(opp, 7, beside).start()
            if t >= 2:
                k = order[t - 2]
                across_relay(k, other).wait_recv()
                if level == 1:
                    make_q(k)
                debias(k, level, prior_ref, raw_c)
                send_back(k)
                if k in mine and k not in late_mine:
                    make_mean(k)
        for k in late_mine:
            make_mean(k)
        for y in range(LEVELS):
            for i in range(GROUP):
                part[y, i] = jnp.sum(acc[y, i], axis=0, keepdims=True)
        for y, o, flip in shares(level):
            share(level, y, o, flip).start()
        spread_in[spread_slot(level, side, r)] = part[level, r]

        across_sent(level)
        drain(raw_a.at[:, nodes(level == 2)], far_send.at[2])
        drain(raw_a.at[pl.ds(0, len(sent_extras)), 0], far_send.at[3])
        drain(raw_b.at[:, nodes(False)], far_send.at[4])
        drain(q_out, far_send.at[5])
        w_copy(level, 3, beside).wait_send()
        w_copy(level, 4, other).wait_send()
        w_copy(beside, 5, other).wait_send()
        w_copy(other, 6, beside).wait_send()
        w_copy(opp, 7, beside).wait_send()
        drain(avgbuf.at[0], avg_send)
        drain(avgbuf.at[1], avg_recv)
        gather_spread(level)
        drain(part, s_send.at[1])
        drain(spread_in.at[pl.ds(0, spread_in.shape[0] - 1)], s_send.at[0])

    def outer_role(level):
        beside, other, opp = NEIGHBOUR[level], 3 - level, (level + 2) % LEVELS
        send_near(first)
        for o in (1, 2, 3):
            w_near(o).start()
        send_near(order[AHEAD:])
        for n, k in enumerate(order):
            if k in first:
                wait_beside(k)
            wait_near(k)
            to_inner(k, beside).start()
            if n == 0:
                near_weights()
                w_copy(level, 3, beside).start()
        w_copy(beside, 3, beside).wait_recv()
        w_copy(opp, 6, beside).wait_recv()
        w_copy(other, 7, beside).wait_recv()
        for k in order:
            outward_relay(k, beside).wait_recv()
            outward_q(k, beside).wait_recv()
            debias(k, level, None, raw_a)
            send_back(k)
        drain(raw_own, far_send.at[0])
        w_copy(level, 3, beside).wait_send()
        drain(avgbuf.at[0], avg_recv)
        gather_spread(level)

    for level in range(LEVELS):
        role = inner_role if level in (1, 2) else outer_role
        pl.when(z == level)(functools.partial(role, level))

    others = pl.ds(0, GROUP - 1)
    drain(raw_own.at[:, others], near_send)
    drain(dbuf.at[:, others], back_send)
    drain(dbuf.at[:, others], back_recv)
    drain(dbuf.at[:, 0], back_own)
    drain(wts.at[0, others], w_send.at[0])
    total = spread_in[0]
    for slot in range(1, spread_in.shape[0]):
        total = total + spread_in[slot]
    spread_ref[0] = jnp.sum(total) / (row_total * hidden)


def fused(params, weights):
    _, rows, hidden = params.shape
    node_count = lax.axis_size("node")
    width = hidden // node_count
    piece_rows = rows // SPLIT
    chunks = LEVELS * SPLIT
    raw = pltpu.VMEM((chunks, GROUP, piece_rows, width), params.dtype)
    q = pltpu.VMEM((chunks, piece_rows, width), jnp.float32)
    dma = pltpu.SemaphoreType.DMA
    debiased, average, spread = pl.pallas_call(
        kernel,
        out_shape=(
            jax.ShapeDtypeStruct((1, rows, hidden), jnp.float32),
            jax.ShapeDtypeStruct((rows, width), jnp.float32),
            jax.ShapeDtypeStruct((1,), jnp.float32),
        ),
        in_specs=[pl.BlockSpec(memory_space=pltpu.HBM), pl.BlockSpec(memory_space=pltpu.SMEM)],
        out_specs=(pl.BlockSpec(memory_space=pl.ANY), pl.BlockSpec(memory_space=pl.ANY),
                   pl.BlockSpec(memory_space=pltpu.SMEM)),
        scratch_shapes=[
            raw, raw, raw, raw, q, q,
            pltpu.VMEM((chunks, GROUP, piece_rows, width), jnp.float32),
            pltpu.VMEM((2, rows, width), jnp.float32),
            pltpu.VMEM((LEVELS, GROUP, 8, LANES), jnp.float32),
            pltpu.VMEM((LEVELS, GROUP, 8, LANES), jnp.float32),
            pltpu.VMEM((LEVELS, GROUP, 1, LANES), jnp.float32),
            pltpu.VMEM((4 * GROUP, 1, LANES), jnp.float32),
            dma, dma((chunks,)), dma((AHEAD,)), dma, dma, dma, dma,
            dma((8,)), dma((chunks,)), dma((chunks,)), dma((chunks,)), dma((chunks,)),
            dma((chunks // 2,)),
            dma((8,)), dma((8,)), dma((2,)), dma, dma, dma,
        ],
        compiler_params=pltpu.CompilerParams(
            collective_id=0, has_side_effects=True, vmem_limit_bytes=20 << 20),
    )(params, weights)
    return debiased, average, spread


def from_behind(value, axis, steps):
    count = lax.axis_size(axis)
    pairs = [(source, (source + steps) % count) for source in range(count)]
    return lax.ppermute(value, axis, pairs)


def push_round(value, scale, hop):
    received = from_behind((value, scale), "node", hop)
    return (received[0], received[1])


def shards(params, weights):
    node_count = lax.axis_size("node")
    levels = node_count.bit_length() - 1
    scale0 = weights.astype(jnp.float32)
    weighted = scale0[:, None, None] * params.astype(jnp.float32)
    value = weighted
    scale = scale0
    for step in range(ROUNDS):
        hop = 1 << step % levels
        if step == 0:
            raw = from_behind((params, weights.astype(jnp.bfloat16)), "node", hop)
            other_scale = raw[1].astype(jnp.float32)
            other_value = other_scale[:, None, None] * raw[0].astype(jnp.float32)
        else:
            other_value, other_scale = push_round(value, scale, hop)
        value = 0.5 * value + 0.5 * other_value
        scale = 0.5 * scale + 0.5 * other_scale
    debiased = value / scale[:, None, None]
    hidden_units = params.shape[2]
    width = hidden_units // node_count
    local = debiased[0]
    numer, total = lax.psum((weighted[0], jnp.sum(scale0)), "node")
    whole = numer / total
    partial_value = jnp.sum((local - whole) ** 2)[None]
    average = lax.dynamic_slice_in_dim(whole, lax.axis_index("node") * width, width, 1)
    row_count = params.shape[1] * lax.axis_size("blk")
    spread = lax.psum(partial_value, "blk") / (row_count * hidden_units)
    return (debiased, average, spread)


def solution(mesh):
    line = mesh.shape["node"] == GROUP * LEVELS and mesh.shape["blk"] == 2
    return jax.shard_map(
        fused if line else shards,
        mesh=mesh,
        in_specs=(P("node", "blk", None), P("node")),
        out_specs=(P("node", "blk", None), P("blk", "node"), P("node")),
        check_vma=False,
    )
```

```python
import functools

import jax
import jax.numpy as jnp
from jax import lax
from jax.experimental import pallas as pl
from jax.experimental.pallas import tpu as pltpu
from jax.sharding import PartitionSpec as P

ROUNDS = 3
GROUP = 4
LEVELS = 4
SPLIT = 4
LANES = 128
FIRST = 2
AHEAD = 2
LATE = 6
NEIGHBOUR = (1, 0, 3, 2)


def kernel(p_ref, w_ref, out_ref, avg_ref, spread_ref,
           raw_own, raw_a, raw_b, raw_c, q_in, q_out, dbuf, avgbuf,
           wts, acc, part, spread_in,
           near_send, near_recv, beside_recv, own_sem, back_send, back_recv, back_own,
           far_send, own_recv, relay_recv, beside_in, q_recv, extra_recv,
           w_send, w_recv, s_send, s_recv, avg_send, avg_recv):
    node = lax.axis_index("node")
    side = lax.axis_index("blk")
    z = node // GROUP
    r = node % GROUP
    half, core = r // 2, r % 2
    chunks, _, rows, width = raw_own.shape
    hidden = p_ref.shape[2]
    row_total = p_ref.shape[1] * lax.axis_size("blk")
    middle = chunks // 2

    lows = list(range(middle))
    highs = list(range(middle + SPLIT, chunks)) + list(range(middle, middle + SPLIT))
    order = [k for pair in zip(lows, highs) for k in pair]
    first = order[:FIRST]

    def peer(o):
        y = 1 - half if o & 2 else half
        c = 1 - core if o & 1 else core
        return y * 2 + c

    def dev(zz, rr):
        return {"node": zz * GROUP + rr}

    inner = jnp.logical_and(z >= 1, z <= 2)
    mate = 3 - z
    nb = (z // 2) * 2 + 1 - z % 2
    inner_count = (1 - z // 3) * ((z + 2) // 3)

    def remote(src, dst, ssem, rsem, device):
        return pltpu.make_async_remote_copy(
            src_ref=src, dst_ref=dst, send_sem=ssem, recv_sem=rsem,
            device_id=device, device_id_type=pl.DeviceIdType.MESH)

    def drain(ref, sem):
        pltpu.make_async_copy(ref, ref, sem).wait()

    def own_slice(k):
        return pl.ds((k % SPLIT) * rows, rows)

    def block(k, rr):
        return pl.ds(pl.multiple_of(((k // SPLIT) * GROUP + rr) * width, LANES), width)

    barrier = pltpu.get_barrier_semaphore()

    def greet(device):
        pl.semaphore_signal(barrier, inc=1, device_id=device,
                            device_id_type=pl.DeviceIdType.MESH)

    for o in (1, 2, 3):
        greet(dev(z, peer(o)))
    greet({"blk": 1 - side})
    greet(dev(nb, r))

    @pl.when(inner)
    def _():
        greet(dev(mate, r))

    def local_in(k):
        return pltpu.make_async_copy(
            p_ref.at[0, own_slice(k), block(k, r)], raw_own.at[k, r], own_sem)

    for k in order:
        local_in(k).start()
    wts[z, r] = jnp.full((8, LANES), w_ref[0].astype(jnp.float32))
    acc[...] = jnp.zeros_like(acc)

    pl.semaphore_wait(barrier, 5 + inner_count)
    drain(raw_own.at[:, 0], own_sem)

    def w_near(o):
        return remote(wts.at[z, r], wts.at[z, r], w_send.at[0], w_recv.at[0],
                      dev(z, peer(o)))

    def near(k, o):
        return remote(p_ref.at[0, own_slice(k), block(k, peer(o))], raw_own.at[k, r],
                      near_send, beside_recv.at[first.index(k)] if k in first and o == 1
                      else near_recv.at[k], dev(z, peer(o)))

    def send_near(ks):
        for k in ks:
            for o in (2, 3, 1):
                near(k, o).start()

    def near_weights():
        drain(wts.at[0, pl.ds(0, GROUP - 1)], w_recv.at[0])

    def wait_beside(k):
        drain(raw_own.at[k, 0], beside_recv.at[first.index(k)])

    def wait_near(k):
        count = GROUP - 2 if k in first else GROUP - 1
        drain(raw_own.at[k, pl.ds(0, count)], near_recv.at[k])

    def row(zz, i):
        return wts[zz, i, 0:1, :]

    def value(ref, k, zz, i, cols):
        return ref[k, i, :, cols].astype(jnp.float32) * row(zz, i)

    def group_sum(ref, k, zz, cols):
        return ((value(ref, k, zz, 0, cols) + value(ref, k, zz, 1, cols))
                + (value(ref, k, zz, 2, cols) + value(ref, k, zz, 3, cols)))

    def columns(j):
        return pl.ds(pl.multiple_of(j * LANES, LANES), LANES)

    def back(k, o):
        return remote(dbuf.at[k, peer(o)], out_ref.at[0, own_slice(k), block(k, r)],
                      back_send, back_recv, dev(z, peer(o)))

    def back_local(k):
        return pltpu.make_async_copy(
            dbuf.at[k, r], out_ref.at[0, own_slice(k), block(k, r)], back_own)

    def send_back(k):
        for o in (2, 3, 1):
            back(k, o).start()
        back_local(k).start()

    def group_weight(zz):
        return row(zz, 0) + row(zz, 1) + row(zz, 2) + row(zz, 3)

    def scales_of(level):
        opp = (level + 2) % LEVELS
        sums = [group_weight((level + 3) % LEVELS)] * GROUP
        for i in range(GROUP):
            for e in range(GROUP):
                sums[i] = sums[i] + row(level if e <= i else opp, e)
        return [1.0 / total for total in sums]

    def window(own, tail, prior):
        heads = [own[0]]
        for i in range(1, GROUP):
            heads.append(heads[-1] + own[i])
        tails = [None, None, None, tail[3]]
        for i in (2, 1):
            tails[i] = tails[i + 1] + tail[i]
        sums = [head + prior for head in heads]
        return [sums[i] + tails[i + 1] for i in range(GROUP - 1)] + [sums[-1]]

    def debias(k, level, prior_ref, tail_ref):
        opp, prior_level = (level + 2) % LEVELS, (level + 3) % LEVELS
        scales = scales_of(level)

        def step(j, carry):
            cols = columns(j)
            if prior_ref is None:
                prior = q_in[k, :, cols]
            else:
                prior = group_sum(prior_ref, k, prior_level, cols)
            own = [value(raw_own, k, level, i, cols) for i in range(GROUP)]
            tail = [None] + [value(tail_ref, k, opp, i, cols) for i in range(1, GROUP)]
            for i, total in enumerate(window(own, tail, prior)):
                dbuf[k, i, :, cols] = total * scales[i]
            return carry

        lax.fori_loop(0, width // LANES, step, 0)

    def means(k, level):
        refs = {level: raw_own, NEIGHBOUR[level]: raw_a, 3 - level: raw_b,
                (level + 2) % LEVELS: raw_c}
        slot = 1 if k // SPLIT == level else 0
        whole = 1.0 / (group_weight(0) + group_weight(1) + group_weight(2) + group_weight(3))
        scales = [scales_of(y) for y in range(LEVELS)]

        def step(j, sums):
            cols = columns(j)
            groups = [group_sum(refs[y], k, y, cols) for y in range(LEVELS)]
            mean = ((groups[0] + groups[1]) + (groups[2] + groups[3])) * whole
            avgbuf[slot, own_slice(k), cols] = mean
            fresh = []
            for y in range(LEVELS):
                far = (y + 2) % LEVELS
                own = [value(refs[y], k, y, i, cols) for i in range(GROUP)]
                tail = [None] + [value(refs[far], k, far, i, cols) for i in range(1, GROUP)]
                for i, total in enumerate(window(own, tail, groups[(y + 3) % LEVELS])):
                    gap = total * scales[y][i] - mean
                    gap = gap * gap
                    fold = gap[0:8]
                    for e in range(8, rows, 8):
                        fold = fold + gap[e:e + 8]
                    fresh.append(sums[y * GROUP + i] + fold)
            return tuple(fresh)

        zero = jnp.zeros((8, LANES), jnp.float32)
        sums = lax.fori_loop(0, width // LANES, step, (zero,) * (LEVELS * GROUP))
        for y in range(LEVELS):
            for i in range(GROUP):
                acc[y, i] += sums[y * GROUP + i]

    def nodes(full):
        return pl.ds(0, GROUP) if full else pl.ds(1, GROUP - 1)

    def to_inner(k, beside):
        return remote(raw_own.at[k], raw_a.at[k], far_send.at[0], beside_in.at[k],
                      dev(beside, r))

    def piece(k, o, source):
        return remote(raw_own.at[k, peer(o)], raw_b.at[k, peer(o)],
                      far_send.at[6 if all_own(k, source) else 7], own_recv.at[k],
                      dev(3 - source, r))

    def all_own(k, source):
        return source == 1 or (k in first and k < middle)

    def pair(k, part_of, source):
        return remote(raw_own.at[k, part_of], raw_b.at[k, part_of],
                      far_send.at[6 if all_own(k, source) else 7], own_recv.at[k],
                      dev(3 - source, r))

    def send_pair(k, chip, source):
        if all_own(k, source):
            pair(k, pl.ds(2 * chip, 2), source).start()
        else:
            pl.when(chip == 0)(pair(k, pl.ds(1, 1), source).start)
            pl.when(chip == 1)(pair(k, pl.ds(2, 2), source).start)

    def across(k, source):
        part_of = nodes(source == 1)
        return remote(raw_own.at[k, part_of], raw_b.at[k, part_of], far_send.at[1],
                      own_recv.at[k], dev(3 - source, r))

    def across_wait(k, source):
        drain(raw_b.at[k, nodes(all_own(k, source))], own_recv.at[k])

    def across_sent(source):
        drain(raw_own.at[pl.ds(0, chunks - FIRST), nodes(source == 1)], far_send.at[1])
        if source == 1:
            drain(raw_own.at[pl.ds(0, FIRST)], far_send.at[6])
        else:
            drain(raw_own.at[pl.ds(0, FIRST // 2)], far_send.at[6])
            drain(raw_own.at[pl.ds(0, FIRST // 2), nodes(False)], far_send.at[7])

    def across_relay(k, source):
        part_of = nodes(source == 2)
        return remote(raw_a.at[k, part_of], raw_c.at[k, part_of], far_send.at[2],
                      relay_recv.at[k], dev(3 - source, r))

    def extra(k, source):
        if source == 1:
            src, dst = raw_a, raw_c
        else:
            src, dst = raw_own, raw_b
        return remote(src.at[k, 0], dst.at[k, 0], far_send.at[3], extra_recv.at[k % middle],
                      dev(3 - source, r))

    def outward_relay(k, source):
        part_of = nodes(False)
        return remote(raw_b.at[k, part_of], raw_a.at[k, part_of], far_send.at[4],
                      beside_in.at[k], dev(NEIGHBOUR[source], r))

    def outward_q(k, source):
        return remote(q_out.at[k], q_in.at[k], far_send.at[5], q_recv.at[k],
                      dev(NEIGHBOUR[source], r))

    def outward_mean(k, source):
        return remote(avgbuf.at[0, own_slice(k)], avg_ref.at[own_slice(k)],
                      avg_send, avg_recv, dev(NEIGHBOUR[source], r))

    def own_mean(k):
        return pltpu.make_async_copy(
            avgbuf.at[1, own_slice(k)], avg_ref.at[own_slice(k)], avg_recv)

    def w_copy(level, slot, target):
        return remote(wts.at[level], wts.at[level], w_send.at[slot], w_recv.at[slot],
                      dev(target, r))

    def spread_slot(level, x, rr):
        return (level - 1) * 2 * GROUP + x * GROUP + rr

    def share(level, y, o, flip):
        x = 1 - side if flip else side
        return remote(part.at[y, peer(o)], spread_in.at[spread_slot(level, side, r)],
                      s_send.at[flip], s_recv,
                      {"node": y * GROUP + peer(o), "blk": x})

    def shares(level):
        return [(y, o, flip) for y in (3 - level, (level + 2) % LEVELS, NEIGHBOUR[level], level)
                for flip in (1, 0) for o in (3, 2, 1, 0) if y != level or flip or o]

    def gather_spread(level):
        slots = spread_in.shape[0]
        drain(spread_in.at[pl.ds(0, slots - 1 if level in (1, 2) else slots)], s_recv)

    def inner_role(level):
        beside, other, opp = NEIGHBOUR[level], 3 - level, (level + 2) % LEVELS
        sent_extras = [k for k in (highs if level == 1 else lows)
                       if level == 1 or k not in first]
        late_sent = sent_extras[-LATE:]
        mine = lows if level == 1 else highs
        late_mine = mine[-LATE:]
        prior_ref = raw_a if level == 1 else raw_b

        def make_q(k):
            src, zz = (raw_c, opp) if level == 1 else (raw_own, level)

            def step(j, carry):
                cols = columns(j)
                q_out[k, :, cols] = group_sum(src, k, zz, cols)
                return carry

            lax.fori_loop(0, width // LANES, step, 0)
            outward_q(k, level).start()

        def make_mean(k):
            if level == 2 or k not in first:
                extra(k, other).wait_recv()
            means(k, level)
            if k // SPLIT == level:
                own_mean(k).start()
            else:
                outward_mean(k, level).start()

        lone = [k for k in first if all_own(k, level)][:FIRST // 2]
        for k in lone:
            piece(k, 0, level).start()
        send_near(first)
        for o in (1, 2, 3):
            w_near(o).start()
        send_near(order[FIRST:])
        for k in first:
            wait_beside(k)
            if k in lone:
                piece(k, 1, level).start()
            else:
                send_pair(k, half, level)
        for n, k in enumerate(first):
            wait_near(k)
            send_pair(k, 1 - half, level)
            if n == 0:
                near_weights()
                w_copy(level, 3, beside).start()
                w_copy(level, 4, other).start()

        for k in order[FIRST:AHEAD]:
            wait_near(k)
            across(k, level).start()
        for t in range(chunks + 2):
            if t + AHEAD < chunks:
                wait_near(order[t + AHEAD])
                across(order[t + AHEAD], level).start()
            if t < chunks:
                k = order[t]
                to_inner(k, beside).wait_recv()
                across_relay(k, level).start()
                if k in sent_extras and k not in late_sent:
                    extra(k, level).start()
                if t == 0:
                    w_copy(beside, 3, beside).wait_recv()
                    w_copy(beside, 5, other).start()
                    w_copy(level, 4, other).wait_recv()
                    w_copy(other, 6, beside).start()
                if t == chunks - 1:
                    for e in late_sent:
                        extra(e, level).start()
                if level == 2:
                    make_q(k)
                across_wait(k, other)
                outward_relay(k, level).start()
            if t == 2:
                w_copy(opp, 5, other).wait_recv()
                w_copy(opp, 7, beside).start()
            if t >= 2:
                k = order[t - 2]
                across_relay(k, other).wait_recv()
                if level == 1:
                    make_q(k)
                debias(k, level, prior_ref, raw_c)
                send_back(k)
                if k in mine and k not in late_mine:
                    make_mean(k)
        for k in late_mine:
            make_mean(k)
        for y in range(LEVELS):
            for i in range(GROUP):
                part[y, i] = jnp.sum(acc[y, i], axis=0, keepdims=True)
        for y, o, flip in shares(level):
            share(level, y, o, flip).start()
        spread_in[spread_slot(level, side, r)] = part[level, r]

        across_sent(level)
        drain(raw_a.at[:, nodes(level == 2)], far_send.at[2])
        drain(raw_a.at[pl.ds(0, len(sent_extras)), 0], far_send.at[3])
        drain(raw_b.at[:, nodes(False)], far_send.at[4])
        drain(q_out, far_send.at[5])
        w_copy(level, 3, beside).wait_send()
        w_copy(level, 4, other).wait_send()
        w_copy(beside, 5, other).wait_send()
        w_copy(other, 6, beside).wait_send()
        w_copy(opp, 7, beside).wait_send()
        drain(avgbuf.at[0], avg_send)
        drain(avgbuf.at[1], avg_recv)
        gather_spread(level)
        drain(part, s_send.at[1])
        drain(spread_in.at[pl.ds(0, spread_in.shape[0] - 1)], s_send.at[0])

    def outer_role(level):
        beside, other, opp = NEIGHBOUR[level], 3 - level, (level + 2) % LEVELS
        send_near(first)
        for o in (1, 2, 3):
            w_near(o).start()
        send_near(order[FIRST:])
        for n, k in enumerate(order):
            if k in first:
                wait_beside(k)
            wait_near(k)
            to_inner(k, beside).start()
            if n == 0:
                near_weights()
                w_copy(level, 3, beside).start()
        w_copy(beside, 3, beside).wait_recv()
        w_copy(opp, 6, beside).wait_recv()
        w_copy(other, 7, beside).wait_recv()
        for k in order:
            outward_relay(k, beside).wait_recv()
            outward_q(k, beside).wait_recv()
            debias(k, level, None, raw_a)
            send_back(k)
        drain(raw_own, far_send.at[0])
        w_copy(level, 3, beside).wait_send()
        drain(avgbuf.at[0], avg_recv)
        gather_spread(level)

    for level in range(LEVELS):
        role = inner_role if level in (1, 2) else outer_role
        pl.when(z == level)(functools.partial(role, level))

    others = pl.ds(0, GROUP - 1)
    drain(raw_own.at[:, others], near_send)
    drain(dbuf.at[:, others], back_send)
    drain(dbuf.at[:, others], back_recv)
    drain(dbuf.at[:, 0], back_own)
    drain(wts.at[0, others], w_send.at[0])
    total = spread_in[0]
    for slot in range(1, spread_in.shape[0]):
        total = total + spread_in[slot]
    spread_ref[0] = jnp.sum(total) / (row_total * hidden)


def fused(params, weights):
    _, rows, hidden = params.shape
    node_count = lax.axis_size("node")
    width = hidden // node_count
    piece_rows = rows // SPLIT
    chunks = LEVELS * SPLIT
    raw = pltpu.VMEM((chunks, GROUP, piece_rows, width), params.dtype)
    q = pltpu.VMEM((chunks, piece_rows, width), jnp.float32)
    dma = pltpu.SemaphoreType.DMA
    debiased, average, spread = pl.pallas_call(
        kernel,
        out_shape=(
            jax.ShapeDtypeStruct((1, rows, hidden), jnp.float32),
            jax.ShapeDtypeStruct((rows, width), jnp.float32),
            jax.ShapeDtypeStruct((1,), jnp.float32),
        ),
        in_specs=[pl.BlockSpec(memory_space=pltpu.HBM), pl.BlockSpec(memory_space=pltpu.SMEM)],
        out_specs=(pl.BlockSpec(memory_space=pl.ANY), pl.BlockSpec(memory_space=pl.ANY),
                   pl.BlockSpec(memory_space=pltpu.SMEM)),
        scratch_shapes=[
            raw, raw, raw, raw, q, q,
            pltpu.VMEM((chunks, GROUP, piece_rows, width), jnp.float32),
            pltpu.VMEM((2, rows, width), jnp.float32),
            pltpu.VMEM((LEVELS, GROUP, 8, LANES), jnp.float32),
            pltpu.VMEM((LEVELS, GROUP, 8, LANES), jnp.float32),
            pltpu.VMEM((LEVELS, GROUP, 1, LANES), jnp.float32),
            pltpu.VMEM((4 * GROUP, 1, LANES), jnp.float32),
            dma, dma((chunks,)), dma((FIRST,)), dma, dma, dma, dma,
            dma((8,)), dma((chunks,)), dma((chunks,)), dma((chunks,)), dma((chunks,)),
            dma((chunks // 2,)),
            dma((8,)), dma((8,)), dma((2,)), dma, dma, dma,
        ],
        compiler_params=pltpu.CompilerParams(
            collective_id=0, has_side_effects=True, vmem_limit_bytes=20 << 20),
    )(pltpu.with_memory_space_constraint(params, pltpu.HBM), weights)
    def place(d_in, a_in, d_out, a_out, sems):
        copies = []
        parts = 8
        step = rows // parts
        for n in range(parts):
            part_of = pl.ds(n * step, step)
            copies.append(pltpu.make_async_copy(
                d_in.at[0, part_of], d_out.at[0, part_of], sems.at[n]))
        copies.append(pltpu.make_async_copy(a_in, a_out, sems.at[parts]))
        for copy in copies:
            copy.start()
        for copy in copies:
            copy.wait()

    debiased, average = pl.pallas_call(
        place,
        out_shape=(jax.ShapeDtypeStruct(debiased.shape, debiased.dtype),
                   jax.ShapeDtypeStruct(average.shape, average.dtype)),
        in_specs=[pl.BlockSpec(memory_space=pl.ANY)] * 2,
        out_specs=(pl.BlockSpec(memory_space=pl.ANY),) * 2,
        scratch_shapes=[dma((9,))],
        compiler_params=pltpu.CompilerParams(vmem_limit_bytes=1 << 20),
    )(debiased, average)
    return debiased, average, spread


def from_behind(value, axis, steps):
    count = lax.axis_size(axis)
    pairs = [(source, (source + steps) % count) for source in range(count)]
    return lax.ppermute(value, axis, pairs)


def push_round(value, scale, hop):
    received = from_behind((value, scale), "node", hop)
    return (received[0], received[1])


def shards(params, weights):
    node_count = lax.axis_size("node")
    levels = node_count.bit_length() - 1
    scale0 = weights.astype(jnp.float32)
    weighted = scale0[:, None, None] * params.astype(jnp.float32)
    value = weighted
    scale = scale0
    for step in range(ROUNDS):
        hop = 1 << step % levels
        if step == 0:
            raw = from_behind((params, weights.astype(jnp.bfloat16)), "node", hop)
            other_scale = raw[1].astype(jnp.float32)
            other_value = other_scale[:, None, None] * raw[0].astype(jnp.float32)
        else:
            other_value, other_scale = push_round(value, scale, hop)
        value = 0.5 * value + 0.5 * other_value
        scale = 0.5 * scale + 0.5 * other_scale
    debiased = value / scale[:, None, None]
    hidden_units = params.shape[2]
    width = hidden_units // node_count
    local = debiased[0]
    numer, total = lax.psum((weighted[0], jnp.sum(scale0)), "node")
    whole = numer / total
    partial_value = jnp.sum((local - whole) ** 2)[None]
    average = lax.dynamic_slice_in_dim(whole, lax.axis_index("node") * width, width, 1)
    row_count = params.shape[1] * lax.axis_size("blk")
    spread = lax.psum(partial_value, "blk") / (row_count * hidden_units)
    return (debiased, average, spread)


def solution(mesh):
    line = mesh.shape["node"] == GROUP * LEVELS and mesh.shape["blk"] == 2
    return jax.shard_map(
        fused if line else shards,
        mesh=mesh,
        in_specs=(P("node", "blk", None), P("node")),
        out_specs=(P("node", "blk", None), P("blk", "node"), P("node")),
        check_vma=False,
    )
```

```python
import functools

import jax
import jax.numpy as jnp
from jax import lax
from jax.experimental import pallas as pl
from jax.experimental.pallas import tpu as pltpu
from jax.sharding import PartitionSpec as P

ROUNDS = 3
GROUP = 4
LEVELS = 4
SPLIT = 4
LANES = 128
FIRST = 2
AHEAD = 2
LATE = (0, 1, 6)
TAPER = 2
NEIGHBOUR = (1, 0, 3, 2)


def kernel(p_ref, w_ref, out_ref, avg_ref, spread_ref,
           raw_own, raw_a, raw_b, raw_c, q_in, q_out, dbuf, avgbuf,
           wts, acc, part, spread_in,
           near_send, near_recv, beside_recv, own_sem, back_send, back_recv,
           far_send, own_recv, relay_recv, beside_in, q_recv, extra_recv,
           w_send, w_recv, s_send, s_recv, avg_send, avg_recv, ready):
    node = lax.axis_index("node")
    side = lax.axis_index("blk")
    z = node // GROUP
    r = node % GROUP
    half, core = r // 2, r % 2
    chunks, _, rows, width = raw_own.shape
    hidden = p_ref.shape[2]
    row_total = p_ref.shape[1] * lax.axis_size("blk")
    middle = chunks // 2

    lows = list(range(middle))
    highs = list(range(middle + SPLIT, chunks)) + list(range(middle, middle + SPLIT))
    order = [k for pair in zip(lows, highs) for k in pair]
    first = order[:FIRST]
    tiles = width // LANES
    cuts = sorted({0, tiles - TAPER * 2, tiles - TAPER, tiles} & set(range(tiles + 1)))

    def units(k):
        if k != order[-1]:
            return [(k, 0, tiles, k)]
        spare = [k] + list(range(chunks, chunks + 2))
        return [(k, lo, hi - lo, sem) for lo, hi, sem in zip(cuts, cuts[1:], spare)]

    def lanes(unit):
        return pl.ds(unit[1] * LANES, unit[2] * LANES)

    def peer(o):
        y = 1 - half if o & 2 else half
        c = 1 - core if o & 1 else core
        return y * 2 + c

    def dev(zz, rr):
        return {"node": zz * GROUP + rr}

    inner = jnp.logical_and(z >= 1, z <= 2)
    mate = 3 - z
    nb = (z // 2) * 2 + 1 - z % 2

    def remote(src, dst, ssem, rsem, device):
        return pltpu.make_async_remote_copy(
            src_ref=src, dst_ref=dst, send_sem=ssem, recv_sem=rsem,
            device_id=device, device_id_type=pl.DeviceIdType.MESH)

    def drain(ref, sem):
        pltpu.make_async_copy(ref, ref, sem).wait()

    def own_slice(k):
        return pl.ds((k % SPLIT) * rows, rows)

    def block(k, rr):
        return pl.ds(pl.multiple_of(((k // SPLIT) * GROUP + rr) * width, LANES), width)

    barrier = pltpu.get_barrier_semaphore()

    def greet(device):
        pl.semaphore_signal(barrier, inc=1, device_id=device,
                            device_id_type=pl.DeviceIdType.MESH)

    for o in (1, 2, 3):
        greet(dev(z, peer(o)))
    greet({"blk": 1 - side})

    @pl.when(inner)
    def _():
        greet(dev(mate, r))
        greet(dev(nb, r))

    def local_in(k):
        return pltpu.make_async_copy(
            p_ref.at[0, own_slice(k), block(k, r)], raw_own.at[k, r], own_sem)

    for k in order:
        local_in(k).start()
    wts[z, r] = jnp.full((8, LANES), w_ref[0].astype(jnp.float32))
    acc[...] = jnp.zeros_like(acc)

    pl.semaphore_wait(barrier, 5)
    drain(raw_own.at[:, 0], own_sem)

    def w_near(o):
        return remote(wts.at[z, r], wts.at[z, r], w_send.at[0], w_recv.at[0],
                      dev(z, peer(o)))

    def near(k, o):
        return remote(p_ref.at[0, own_slice(k), block(k, peer(o))], raw_own.at[k, r],
                      near_send, beside_recv.at[first.index(k)] if k in first and o == 1
                      else near_recv.at[k], dev(z, peer(o)))

    def send_near(ks):
        for k in ks:
            for o in (2, 3, 1):
                near(k, o).start()

    def near_weights():
        drain(wts.at[0, pl.ds(0, GROUP - 1)], w_recv.at[0])

    def wait_beside(k):
        drain(raw_own.at[k, 0], beside_recv.at[first.index(k)])

    def wait_near(k):
        count = GROUP - 2 if k in first else GROUP - 1
        drain(raw_own.at[k, pl.ds(0, count)], near_recv.at[k])

    def row(zz, i):
        return wts[zz, i, 0:1, :]

    def value(ref, k, zz, i, cols):
        return ref[k, i, :, cols].astype(jnp.float32) * row(zz, i)

    def group_sum(ref, k, zz, cols):
        return ((value(ref, k, zz, 0, cols) + value(ref, k, zz, 1, cols))
                + (value(ref, k, zz, 2, cols) + value(ref, k, zz, 3, cols)))

    def columns(j):
        return pl.ds(pl.multiple_of(j * LANES, LANES), LANES)

    def out_block(unit):
        k, lo, count, _ = unit
        start = ((k // SPLIT) * GROUP + r) * width + lo * LANES
        return out_ref.at[0, own_slice(k), pl.ds(pl.multiple_of(start, LANES), count * LANES)]

    def back(unit, o):
        return remote(dbuf.at[unit[0], peer(o), :, lanes(unit)], out_block(unit),
                      back_send, back_recv, dev(z, peer(o)))

    def send_back(unit):
        for o in (2, 3, 1):
            back(unit, o).start()

    def group_weight(zz):
        return row(zz, 0) + row(zz, 1) + row(zz, 2) + row(zz, 3)

    def scales_of(level):
        opp = (level + 2) % LEVELS
        sums = [group_weight((level + 3) % LEVELS)] * GROUP
        for i in range(GROUP):
            for e in range(GROUP):
                sums[i] = sums[i] + row(level if e <= i else opp, e)
        return [1.0 / total for total in sums]

    def window(own, tail, prior):
        heads = [own[0]]
        for i in range(1, GROUP):
            heads.append(heads[-1] + own[i])
        tails = [None, None, None, tail[3]]
        for i in (2, 1):
            tails[i] = tails[i + 1] + tail[i]
        sums = [head + prior for head in heads]
        return [sums[i] + tails[i + 1] for i in range(GROUP - 1)] + [sums[-1]]

    def debias(unit, level, prior_ref, tail_ref):
        k, lo, count, _ = unit
        opp, prior_level = (level + 2) % LEVELS, (level + 3) % LEVELS
        scales = scales_of(level)

        def step(j, carry):
            cols = columns(j)
            if prior_ref is None:
                prior = q_in[k, :, cols]
            else:
                prior = group_sum(prior_ref, k, prior_level, cols)
            own = [value(raw_own, k, level, i, cols) for i in range(GROUP)]
            tail = [None] + [value(tail_ref, k, opp, i, cols) for i in range(1, GROUP)]
            for i, total in enumerate(window(own, tail, prior)):
                dbuf[k, i, :, cols] = total * scales[i]
            start = ((k // SPLIT) * GROUP + r) * width + j * LANES
            place = pl.ds(pl.multiple_of(start, LANES), LANES)
            out_ref[0, own_slice(k), place] = dbuf[k, r, :, cols]
            return carry

        lax.fori_loop(lo, lo + count, step, 0)

    def means(k, level):
        refs = {level: raw_own, NEIGHBOUR[level]: raw_a, 3 - level: raw_b,
                (level + 2) % LEVELS: raw_c}
        own_average = k // SPLIT == level
        whole = 1.0 / (group_weight(0) + group_weight(1) + group_weight(2) + group_weight(3))
        scales = [scales_of(y) for y in range(LEVELS)]

        def step(j, sums):
            cols = columns(j)
            groups = [group_sum(refs[y], k, y, cols) for y in range(LEVELS)]
            mean = ((groups[0] + groups[1]) + (groups[2] + groups[3])) * whole
            (avg_ref if own_average else avgbuf)[own_slice(k), cols] = mean
            fresh = []
            for y in range(LEVELS):
                far = (y + 2) % LEVELS
                if y == level:
                    results = [dbuf[k, i, :, cols] for i in range(GROUP)]
                else:
                    own = [value(refs[y], k, y, i, cols) for i in range(GROUP)]
                    tail = [None] + [value(refs[far], k, far, i, cols) for i in range(1, GROUP)]
                    totals = window(own, tail, groups[(y + 3) % LEVELS])
                    results = [total * scale for total, scale in zip(totals, scales[y])]
                for i in range(GROUP):
                    gap = results[i] - mean
                    gap = gap * gap
                    fold = gap[0:8]
                    for e in range(8, rows, 8):
                        fold = fold + gap[e:e + 8]
                    fresh.append(sums[y * GROUP + i] + fold)
            return tuple(fresh)

        zero = jnp.zeros((8, LANES), jnp.float32)
        sums = lax.fori_loop(0, width // LANES, step, (zero,) * (LEVELS * GROUP))
        for y in range(LEVELS):
            for i in range(GROUP):
                acc[y, i] += sums[y * GROUP + i]

    def nodes(full):
        return pl.ds(0, GROUP) if full else pl.ds(1, GROUP - 1)

    def to_inner(k, beside):
        return remote(raw_own.at[k], raw_a.at[k], far_send.at[0], beside_in.at[k],
                      dev(beside, r))

    def piece(k, o, source):
        return remote(raw_own.at[k, peer(o)], raw_b.at[k, peer(o)],
                      far_send.at[6 if all_own(k, source) else 7], own_recv.at[k],
                      dev(3 - source, r))

    def all_own(k, source):
        return source == 1 or (k in first and k < middle)

    def pair(k, part_of, source):
        return remote(raw_own.at[k, part_of], raw_b.at[k, part_of],
                      far_send.at[6 if all_own(k, source) else 7], own_recv.at[k],
                      dev(3 - source, r))

    def send_pair(k, chip, source):
        if all_own(k, source):
            pair(k, pl.ds(2 * chip, 2), source).start()
        else:
            pl.when(chip == 0)(pair(k, pl.ds(1, 1), source).start)
            pl.when(chip == 1)(pair(k, pl.ds(2, 2), source).start)

    def across(k, source):
        part_of = nodes(source == 1)
        return remote(raw_own.at[k, part_of], raw_b.at[k, part_of], far_send.at[1],
                      own_recv.at[k], dev(3 - source, r))

    def across_wait(k, source):
        drain(raw_b.at[k, nodes(all_own(k, source))], own_recv.at[k])

    def across_sent(source):
        drain(raw_own.at[pl.ds(0, chunks - FIRST), nodes(source == 1)], far_send.at[1])
        if source == 1:
            drain(raw_own.at[pl.ds(0, FIRST)], far_send.at[6])
        else:
            drain(raw_own.at[pl.ds(0, FIRST // 2)], far_send.at[6])
            drain(raw_own.at[pl.ds(0, FIRST // 2), nodes(False)], far_send.at[7])

    def across_relay(unit, source):
        place = (unit[0], nodes(source == 2), slice(None), lanes(unit))
        return remote(raw_a.at[place], raw_c.at[place], far_send.at[2],
                      relay_recv.at[unit[3]], dev(3 - source, r))

    def extra(k, source):
        if source == 1:
            src, dst = raw_a, raw_c
        else:
            src, dst = raw_own, raw_b
        return remote(src.at[k, 0], dst.at[k, 0], far_send.at[3], extra_recv.at[k % middle],
                      dev(3 - source, r))

    def outward_relay(k, source):
        part_of = nodes(False)
        return remote(raw_b.at[k, part_of], raw_a.at[k, part_of], far_send.at[4],
                      beside_in.at[k], dev(NEIGHBOUR[source], r))

    def outward_q(unit, source):
        place = (unit[0], slice(None), lanes(unit))
        return remote(q_out.at[place], q_in.at[place], far_send.at[5],
                      q_recv.at[unit[3]], dev(NEIGHBOUR[source], r))

    def outward_mean(k, source):
        return remote(avgbuf.at[own_slice(k)], avg_ref.at[own_slice(k)],
                      avg_send, avg_recv, dev(NEIGHBOUR[source], r))

    def w_copy(level, slot, target):
        return remote(wts.at[level], wts.at[level], w_send.at[slot], w_recv.at[slot],
                      dev(target, r))

    def spread_slot(level, x, rr):
        return (level - 1) * 2 * GROUP + x * GROUP + rr

    def share(level, y, o, flip):
        x = 1 - side if flip else side
        return remote(part.at[y, peer(o)], spread_in.at[spread_slot(level, side, r)],
                      s_send.at[flip], s_recv,
                      {"node": y * GROUP + peer(o), "blk": x})

    def shares(level):
        return [(y, o, flip) for y in (3 - level, (level + 2) % LEVELS, NEIGHBOUR[level], level)
                for flip in (1, 0) for o in (3, 2, 1, 0) if y != level or flip or o]

    def gather_spread(level):
        slots = spread_in.shape[0]
        drain(spread_in.at[pl.ds(0, slots - 1 if level in (1, 2) else slots)], s_recv)

    def inner_role(level):
        beside, other, opp = NEIGHBOUR[level], 3 - level, (level + 2) % LEVELS
        sent_extras = [k for k in (highs if level == 1 else lows)
                       if level == 1 or k not in first]
        late_sent = sent_extras[len(sent_extras) - LATE[level]:]
        mine = lows if level == 1 else highs
        late_mine = mine[len(mine) - LATE[other]:]
        prior_ref = raw_a if level == 1 else raw_b

        def make_q(unit):
            k, lo, count, _ = unit
            src, zz = (raw_c, opp) if level == 1 else (raw_own, level)

            def step(j, carry):
                cols = columns(j)
                q_out[k, :, cols] = group_sum(src, k, zz, cols)
                return carry

            lax.fori_loop(lo, lo + count, step, 0)
            outward_q(unit, level).start()

        def make_mean(k):
            if level == 2 or k not in first:
                extra(k, other).wait_recv()
            means(k, level)
            if k // SPLIT != level:
                outward_mean(k, level).start()

        lone = [k for k in first if all_own(k, level)][:FIRST // 2]
        for k in lone:
            piece(k, 0, level).start()
        send_near(first)
        for o in (1, 2, 3):
            w_near(o).start()
        send_near(order[FIRST:])
        for k in first:
            wait_beside(k)
            if k in lone:
                piece(k, 1, level).start()
            else:
                send_pair(k, half, level)
        for n, k in enumerate(first):
            wait_near(k)
            send_pair(k, 1 - half, level)
            if n == 0:
                near_weights()
                w_copy(level, 4, other).start()

        for k in order[FIRST:AHEAD]:
            wait_near(k)
            across(k, level).start()
        for t in range(chunks + 2):
            if t + AHEAD < chunks:
                wait_near(order[t + AHEAD])
                across(order[t + AHEAD], level).start()
            if t < chunks:
                k = order[t]
                to_inner(k, beside).wait_recv()
                for unit in units(k):
                    across_relay(unit, level).start()
                if k in sent_extras and k not in late_sent:
                    extra(k, level).start()
                if t == 0:
                    pl.semaphore_wait(ready, 1)
                    w_copy(level, 3, beside).start()
                    w_copy(beside, 3, beside).wait_recv()
                    w_copy(beside, 5, other).start()
                    w_copy(level, 4, other).wait_recv()
                    w_copy(other, 6, beside).start()
                if t == chunks - 1:
                    for e in late_sent:
                        extra(e, level).start()
                if level == 2:
                    for unit in units(k):
                        make_q(unit)
                across_wait(k, other)
                outward_relay(k, level).start()
            if t == 2:
                w_copy(opp, 5, other).wait_recv()
                w_copy(opp, 7, beside).start()
            if t >= 2:
                k = order[t - 2]
                for unit in units(k):
                    across_relay(unit, other).wait_recv()
                    if level == 1:
                        make_q(unit)
                    debias(unit, level, prior_ref, raw_c)
                    send_back(unit)
                if k in mine and k not in late_mine:
                    make_mean(k)
        for k in late_mine:
            make_mean(k)
        for y in range(LEVELS):
            for i in range(GROUP):
                part[y, i] = jnp.sum(acc[y, i], axis=0, keepdims=True)
        for y, o, flip in shares(level):
            share(level, y, o, flip).start()
        spread_in[spread_slot(level, side, r)] = part[level, r]

        across_sent(level)
        drain(raw_a.at[:, nodes(level == 2)], far_send.at[2])
        drain(raw_a.at[pl.ds(0, len(sent_extras)), 0], far_send.at[3])
        drain(raw_b.at[:, nodes(False)], far_send.at[4])
        drain(q_out, far_send.at[5])
        w_copy(level, 3, beside).wait_send()
        w_copy(level, 4, other).wait_send()
        w_copy(beside, 5, other).wait_send()
        w_copy(other, 6, beside).wait_send()
        w_copy(opp, 7, beside).wait_send()
        drain(avgbuf, avg_send)
        gather_spread(level)
        drain(part, s_send.at[1])
        drain(spread_in.at[pl.ds(0, spread_in.shape[0] - 1)], s_send.at[0])

    def outer_role(level):
        beside, other, opp = NEIGHBOUR[level], 3 - level, (level + 2) % LEVELS
        pl.semaphore_signal(ready, inc=1, device_id=dev(beside, r),
                            device_id_type=pl.DeviceIdType.MESH)
        send_near(first)
        for o in (1, 2, 3):
            w_near(o).start()
        send_near(order[FIRST:])
        for n, k in enumerate(order):
            if k in first:
                wait_beside(k)
            wait_near(k)
            to_inner(k, beside).start()
            if n == 0:
                near_weights()
                w_copy(level, 3, beside).start()
        w_copy(beside, 3, beside).wait_recv()
        w_copy(opp, 6, beside).wait_recv()
        w_copy(other, 7, beside).wait_recv()
        for k in order:
            outward_relay(k, beside).wait_recv()
            for unit in units(k):
                outward_q(unit, beside).wait_recv()
                debias(unit, level, None, raw_a)
                send_back(unit)
        drain(raw_own, far_send.at[0])
        w_copy(level, 3, beside).wait_send()
        drain(avgbuf, avg_recv)
        gather_spread(level)

    for level in range(LEVELS):
        role = inner_role if level in (1, 2) else outer_role
        pl.when(z == level)(functools.partial(role, level))

    others = pl.ds(0, GROUP - 1)
    drain(raw_own.at[:, others], near_send)
    drain(dbuf.at[:, others], back_send)
    drain(dbuf.at[:, others], back_recv)
    drain(wts.at[0, others], w_send.at[0])
    total = spread_in[0]
    for slot in range(1, spread_in.shape[0]):
        total = total + spread_in[slot]
    spread_ref[0] = jnp.sum(total) / (row_total * hidden)


def fused(params, weights):
    _, rows, hidden = params.shape
    node_count = lax.axis_size("node")
    width = hidden // node_count
    piece_rows = rows // SPLIT
    chunks = LEVELS * SPLIT
    raw = pltpu.VMEM((chunks, GROUP, piece_rows, width), params.dtype)
    q = pltpu.VMEM((chunks, piece_rows, width), jnp.float32)
    dma = pltpu.SemaphoreType.DMA
    debiased, average, spread = pl.pallas_call(
        kernel,
        out_shape=(
            jax.ShapeDtypeStruct((1, rows, hidden), jnp.float32),
            jax.ShapeDtypeStruct((rows, width), jnp.float32),
            jax.ShapeDtypeStruct((1,), jnp.float32),
        ),
        in_specs=[pl.BlockSpec(memory_space=pltpu.HBM), pl.BlockSpec(memory_space=pltpu.SMEM)],
        out_specs=(pl.BlockSpec(memory_space=pltpu.VMEM), pl.BlockSpec(memory_space=pltpu.VMEM),
                   pl.BlockSpec(memory_space=pltpu.SMEM)),
        scratch_shapes=[
            raw, raw, raw, raw, q, q,
            pltpu.VMEM((chunks, GROUP, piece_rows, width), jnp.float32),
            pltpu.VMEM((rows, width), jnp.float32),
            pltpu.VMEM((LEVELS, GROUP, 8, LANES), jnp.float32),
            pltpu.VMEM((LEVELS, GROUP, 8, LANES), jnp.float32),
            pltpu.VMEM((LEVELS, GROUP, 1, LANES), jnp.float32),
            pltpu.VMEM((4 * GROUP, 1, LANES), jnp.float32),
            dma, dma((chunks,)), dma((FIRST,)), dma, dma, dma,
            dma((8,)), dma((chunks,)), dma((chunks + 2,)), dma((chunks,)), dma((chunks + 2,)),
            dma((chunks // 2,)),
            dma((8,)), dma((8,)), dma((2,)), dma, dma, dma,
            pltpu.SemaphoreType.REGULAR,
        ],
        compiler_params=pltpu.CompilerParams(
            collective_id=0, has_side_effects=True, vmem_limit_bytes=20 << 20),
    )(pltpu.with_memory_space_constraint(params, pltpu.HBM), weights)
    def place(d_in, a_in, d_out, a_out, sems):
        copies = []
        parts = 8
        step = rows // parts
        for n in range(parts):
            part_of = pl.ds(n * step, step)
            copies.append(pltpu.make_async_copy(
                d_in.at[0, part_of], d_out.at[0, part_of], sems.at[n]))
        copies.append(pltpu.make_async_copy(a_in, a_out, sems.at[parts]))
        for copy in copies:
            copy.start()
        for copy in copies:
            copy.wait()

    debiased, average = pl.pallas_call(
        place,
        out_shape=(jax.ShapeDtypeStruct(debiased.shape, debiased.dtype),
                   jax.ShapeDtypeStruct(average.shape, average.dtype)),
        in_specs=[pl.BlockSpec(memory_space=pl.ANY)] * 2,
        out_specs=(pl.BlockSpec(memory_space=pl.ANY),) * 2,
        scratch_shapes=[dma((9,))],
        compiler_params=pltpu.CompilerParams(vmem_limit_bytes=1 << 20),
    )(debiased, average)
    return debiased, average, spread


def from_behind(value, axis, steps):
    count = lax.axis_size(axis)
    pairs = [(source, (source + steps) % count) for source in range(count)]
    return lax.ppermute(value, axis, pairs)


def push_round(value, scale, hop):
    received = from_behind((value, scale), "node", hop)
    return (received[0], received[1])


def shards(params, weights):
    node_count = lax.axis_size("node")
    levels = node_count.bit_length() - 1
    scale0 = weights.astype(jnp.float32)
    weighted = scale0[:, None, None] * params.astype(jnp.float32)
    value = weighted
    scale = scale0
    for step in range(ROUNDS):
        hop = 1 << step % levels
        if step == 0:
            raw = from_behind((params, weights.astype(jnp.bfloat16)), "node", hop)
            other_scale = raw[1].astype(jnp.float32)
            other_value = other_scale[:, None, None] * raw[0].astype(jnp.float32)
        else:
            other_value, other_scale = push_round(value, scale, hop)
        value = 0.5 * value + 0.5 * other_value
        scale = 0.5 * scale + 0.5 * other_scale
    debiased = value / scale[:, None, None]
    hidden_units = params.shape[2]
    width = hidden_units // node_count
    local = debiased[0]
    numer, total = lax.psum((weighted[0], jnp.sum(scale0)), "node")
    whole = numer / total
    partial_value = jnp.sum((local - whole) ** 2)[None]
    average = lax.dynamic_slice_in_dim(whole, lax.axis_index("node") * width, width, 1)
    row_count = params.shape[1] * lax.axis_size("blk")
    spread = lax.psum(partial_value, "blk") / (row_count * hidden_units)
    return (debiased, average, spread)


def solution(mesh):
    line = mesh.shape["node"] == GROUP * LEVELS and mesh.shape["blk"] == 2
    return jax.shard_map(
        fused if line else shards,
        mesh=mesh,
        in_specs=(P("node", "blk", None), P("node")),
        out_specs=(P("node", "blk", None), P("blk", "node"), P("node")),
        check_vma=False,
    )
```
